256 devices in a mesh: row: 8 (over x, z_hi), col: 32 (over y, z_lo, core).
Axes of the slice: x: 4, y: 4, z: 8 (z_hi: 2, z_lo: 4; z = z_hi * 4 + z_lo), core: 2. Of those that a mesh axis runs over, the one named last changes fastest.
Arguments:
- chol_window: bfloat16 [512, 8, 1024], P('row', None, 'col'), may hold values from -6 to 6
- pair_vectors: bfloat16 [512, 512, 1024], P('row', 'col'), may hold values from -0.1875 to 0.1875
- amplitudes: bfloat16 [512, 512, 256], P('row', 'col'), may hold values from -0.0234375 to 0.0234375
Outputs:
- ladder: float32 [8, 256, 512], P(None, 'col', 'row')
The draws below stay inside these ranges and needn't reach their ends.
All inputs are finite; a program needn't handle non-finite values.
Results may differ from the reference program's by a relative error of at most 0.0029.
Values may be sent and summed in bfloat16 or wider, within the bound.
No kernel may reach another device: no remote copies, remote signals or barrier semaphores. Data moves between devices by JAX's collectives and lax.ppermute only.
A program may use at most 128 MiB of HBM per device.

```python
import jax
import jax.numpy as jnp
from jax import lax

V = 512
NQ = 1024
NA = 8
NP = 256


def strengthened(result, rng, source, target, shards_of, factor):
    def block_of(axis_at):
        return (jnp.arange(result.shape[axis_at]) // (result.shape[axis_at] // shards_of)).reshape((-1,) + (1,) * (result.ndim - 1 - axis_at))

    first = jax.random.permutation(rng, shards_of)[block_of(target)]
    second = (block_of(target) + shards_of // 2) % shards_of
    return jnp.where((block_of(source) == first) | (block_of(source) == second), factor * result, result)


def shard_levels(rng, dims, pieces, low, largest):
    def one(position, blocks):
        draws = jax.random.uniform(jax.random.fold_in(jax.random.fold_in(rng, 6), position), (blocks,), jnp.float32, low / len(pieces), largest / len(pieces))
        return jnp.repeat(jnp.exp(draws), dims[position] // blocks).reshape((-1,) + (1,) * (len(dims) - position - 1))

    level = one(*pieces[0])
    for cut in pieces[1:]:
        level = level * one(*cut)
    return level


def centred(key, shape, spread, bound, pieces=(), dtype=jnp.bfloat16):
    level = shard_levels(key, shape, pieces, -0.22, 0.18) if pieces else 1.0
    array = jax.random.normal(key, shape, jnp.float32) * spread * level
    return jnp.minimum(jnp.maximum(array, -bound), bound).astype(dtype)


def gaussian_with(key, dims, deviation, limit, shards, heavy, dtype=jnp.bfloat16):
    drawn = deviation * jax.random.normal(key, dims, jnp.float32)
    if shards:
        drawn = drawn * shard_levels(key, dims, shards, -0.22, 0.18)
    return jnp.clip(strengthened(drawn, jax.random.fold_in(key, 3), *heavy), -limit, limit).astype(dtype)


def setup_inputs(seed: int = 0) -> dict:
    key_of = jax.random.split(jax.random.key(seed), 4)
    chol_window = centred(key_of[0], (V, NA, NQ), 1.0, 6.0, ((0, 8), (2, 32)))
    pair_vectors = centred(key_of[1], (V, V, NQ), NQ ** -0.5, 0.1875, ((0, 8), (1, 32)))
    amplitudes = gaussian_with(key_of[2], (V, V, NP), (V * V) ** -0.5, 0.0234375, ((0, 8), (1, 32)), (1, 2, 32, 2.75))
    return dict(chol_window=chol_window, pair_vectors=pair_vectors, amplitudes=amplitudes)


def reference(chol_window, pair_vectors, amplitudes):
    block_rows = 16
    flat_window = chol_window.reshape(V * NA, NQ)
    stacked = pair_vectors.reshape(V // block_rows, block_rows * V, NQ)
    amps_wide = amplitudes.astype(jnp.float32)

    def one_block(vectors):
        integrals = lax.dot_general(flat_window, vectors, (((1,), (1,)), ((), ())), preferred_element_type=jnp.float32)
        integrals = integrals.astype(jnp.bfloat16).astype(jnp.float32).reshape(V, NA, block_rows, V)
        return jnp.einsum("cabd,cdn->anb", integrals, amps_wide, precision=lax.Precision.HIGHEST)

    pieces_out = lax.map(one_block, stacked)
    return pieces_out.transpose(1, 2, 0, 3).reshape(NA, NP, V)
```

```python
import jax
import jax.numpy as jnp
from jax import lax
from jax.experimental import pallas as pl
from jax.experimental.pallas import tpu as pltpu
from jax.sharding import PartitionSpec as P

X, ZH, Y, ZL, CORE = 4, 2, 4, 4, 2
Z = ZH * ZL
COLS = Y * ZL * CORE
PARTIAL = jnp.bfloat16
GROUPS = ((0, 1, 7), (2, 6, 3, 5, 4))


def linear(x, zh, y, zl, core):
    return (((x % X * ZH + zh % ZH) * Y + y % Y) * ZL + zl % ZL) * CORE + core % CORE


def fetch(array, dx=0, dy=0, dz=0, dcore=0):
    perm = []
    for x in range(X):
        for z in range(Z):
            for y in range(Y):
                for core in range(CORE):
                    far = (z + dz) % Z
                    perm.append((
                        linear(x + dx, far // ZL, y + dy, far % ZL, core + dcore),
                        linear(x, z // ZL, y, z % ZL, core),
                    ))
    return lax.ppermute(array, ("row", "col"), perm)


def place():
    row, col = lax.axis_index("row"), lax.axis_index("col")
    return lax.rem(row, ZH), col // (ZL * CORE), lax.rem(col // CORE, ZL), lax.rem(col, CORE)


def integrals_kernel(*refs):
    pieces, (vectors_ref, out_ref) = refs[:-2], refs[-2:]
    zh, _, zl, _ = place()
    swapped = [lax.rem((zh * ZL + zl + step) // ZL, ZH) != 0 for step in range(ZL)]
    rows = []
    for pair in range(CORE * Y):
        held = {}
        for g, group in enumerate(GROUPS):
            for i, dz in enumerate(group):
                held[dz] = pieces[pair * len(GROUPS) + g][i, 0]
        for step in range(ZL):
            near, far = held[step], held[step + ZL]
            low = jnp.where(swapped[step], far, near)
            high = jnp.where(swapped[step], near, far)
            rows.append(jnp.concatenate([low, high], axis=1))
    window = jnp.concatenate(rows, axis=0)
    block = jnp.dot(vectors_ref[...], window, preferred_element_type=jnp.float32)
    out_ref[...] = block.astype(out_ref.dtype)


def integrals_of(pieces, vectors):
    _, n_a, q_own, c_half = pieces[0].shape
    rows, n_q = vectors.shape
    n_c = c_half * ZH
    specs = [
        pl.BlockSpec((piece.shape[0], 1, q_own, c_half), lambda a: (0, a, 0, 0)) for piece in pieces
    ]
    return pl.pallas_call(
        integrals_kernel,
        grid=(n_a,),
        out_shape=jax.ShapeDtypeStruct((rows, n_a * n_c), jnp.bfloat16),
        in_specs=specs + [pl.BlockSpec((rows, n_q), lambda a: (0, 0))],
        out_specs=pl.BlockSpec((rows, n_c), lambda a: (0, a)),
        compiler_params=pltpu.CompilerParams(vmem_limit_bytes=24 << 20),
        cost_estimate=pl.CostEstimate(
            flops=2 * rows * n_q * n_a * n_c, transcendentals=0,
            bytes_accessed=2 * (n_q * n_a * n_c + rows * n_q + rows * n_a * n_c),
        ),
    )(*pieces, vectors)


def ladder_kernel(*refs, n_a, n_b, n_c, d_block):
    amps, (integrals_ref, out_ref, acc_ref) = refs[:-3], refs[-3:]
    zh = place()[0]
    block = pl.program_id(0)

    @pl.when(block == 0)
    def _():
        acc_ref[...] = jnp.zeros_like(acc_ref)

    total = acc_ref[...]
    for d in range(d_block):
        near = jnp.concatenate([amps[i][d] for i in range(X)], axis=0)
        far = jnp.concatenate([amps[X + i][d] for i in range(X)], axis=0)
        low, high = jnp.where(zh != 0, far, near), jnp.where(zh != 0, near, far)
        amplitudes = jnp.concatenate([low, high], axis=0)
        stacked = jnp.concatenate(
            [integrals_ref[d * n_b:(d + 1) * n_b, a * n_c:(a + 1) * n_c] for a in range(n_a)], axis=0)
        total += jnp.dot(stacked, amplitudes, preferred_element_type=jnp.float32)
    acc_ref[...] = total

    @pl.when(block == pl.num_programs(0) - 1)
    def _():
        out_ref[...] = acc_ref[...].T.astype(out_ref.dtype)


def ladder_of(integrals, amps, n_a, d_block=4):
    n_d, c_own, n_n = amps[0].shape
    n_c = c_own * X * ZH
    n_b = integrals.shape[0] // n_d

    def kernel(*refs):
        ladder_kernel(*refs, n_a=n_a, n_b=n_b, n_c=n_c, d_block=d_block)

    return pl.pallas_call(
        kernel,
        grid=(n_d // d_block,),
        out_shape=jax.ShapeDtypeStruct((n_n, n_a * n_b), PARTIAL),
        in_specs=[pl.BlockSpec((d_block, c_own, n_n), lambda d: (d, 0, 0))] * len(amps)
        + [pl.BlockSpec((d_block * n_b, n_a * n_c), lambda d: (d, 0))],
        out_specs=pl.BlockSpec((n_n, n_a * n_b), lambda d: (0, 0)),
        scratch_shapes=[pltpu.VMEM((n_a * n_b, n_n), jnp.float32)],
        compiler_params=pltpu.CompilerParams(vmem_limit_bytes=24 << 20),
        cost_estimate=pl.CostEstimate(
            flops=2 * n_d * n_b * n_a * n_c * n_n, transcendentals=0,
            bytes_accessed=2 * (n_d * n_c * n_n + n_d * n_b * n_a * n_c),
        ),
    )(*amps, integrals)


def ordered_vectors(pair_vectors):
    n_b, n_d, n_q = pair_vectors.shape
    _, y, zl, core = place()
    own = n_q // COLS
    position = jnp.arange(n_q)
    far, q = position // own, position % own
    dzl, dy, dcore = far % ZL, far // ZL % Y, far // (ZL * Y)
    source = (((y + dy) % Y * ZL + (zl + dzl) % ZL) * CORE + (core + dcore) % CORE) * own + q
    picked = (jnp.arange(n_q)[:, None] == source[None, :]).astype(pair_vectors.dtype)
    moved = pair_vectors.transpose(1, 0, 2).reshape(n_d * n_b, n_q)
    return jnp.dot(moved, picked, preferred_element_type=jnp.float32).astype(pair_vectors.dtype)


def gathered_window(window):
    mine = window.transpose(1, 2, 0)
    near = [mine] + [fetch(mine, dx=dx) for dx in range(1, X)]
    parts = jnp.concatenate(near, axis=2)
    along_z = [parts] + [fetch(parts, dz=dz) for dz in range(1, Z)]
    groups = [jnp.stack([along_z[dz] for dz in group]) for group in GROUPS]
    along_y = [[group] + [fetch(group, dy=dy) for dy in range(1, Y)] for group in groups]
    both = [along_y] + [[[fetch(part, dcore=1) for part in parts_y] for parts_y in along_y]]
    return [both[dcore][g][dy] for dcore in range(CORE) for dy in range(Y) for g in range(len(GROUPS))]


def local(chol_window, pair_vectors, amplitudes):
    n_b = pair_vectors.shape[0]
    n_a = chol_window.shape[1]
    n_n = amplitudes.shape[2]
    pieces = gathered_window(chol_window)
    amps_mine = amplitudes.transpose(1, 0, 2)
    amps_near = [amps_mine] + [fetch(amps_mine, dx=dx) for dx in range(1, X)]
    amps_swap = fetch(amps_mine, dz=ZL)
    amps_far = [amps_swap] + [fetch(amps_swap, dx=dx) for dx in range(1, X)]
    integrals = integrals_of(pieces, ordered_vectors(pair_vectors))
    partial = ladder_of(integrals, amps_near + amps_far, n_a)
    tiles = lax.all_to_all(partial.reshape(COLS, n_n // COLS, n_a * n_b), "col", 0, 0, tiled=True)
    total = jnp.sum(tiles.astype(jnp.float32), axis=0)
    return total.reshape(n_n // COLS, n_a, n_b).transpose(1, 0, 2)


def solution(mesh):
    return jax.shard_map(
        local,
        mesh=mesh,
        in_specs=(P("row", None, "col"), P("row", "col", None), P("row", "col", None)),
        out_specs=P(None, "col", "row"),
        check_vma=False,
    )
```

```python
import jax
import jax.numpy as jnp
from jax import lax
from jax.experimental import pallas as pl
from jax.experimental.pallas import tpu as pltpu
from jax.sharding import PartitionSpec as P

X, ZH, Y, ZL, CORE = 4, 2, 4, 4, 2
Z = ZH * ZL
COLS = Y * ZL * CORE
PARTIAL = jnp.bfloat16
GROUPS = ((0,), (1, 7), (2, 6), (3, 5, 4))


def linear(x, zh, y, zl, core):
    return (((x % X * ZH + zh % ZH) * Y + y % Y) * ZL + zl % ZL) * CORE + core % CORE


def fetch(array, dx=0, dy=0, dz=0, dcore=0):
    perm = []
    for x in range(X):
        for z in range(Z):
            for y in range(Y):
                for core in range(CORE):
                    far = (z + dz) % Z
                    perm.append((
                        linear(x + dx, far // ZL, y + dy, far % ZL, core + dcore),
                        linear(x, z // ZL, y, z % ZL, core),
                    ))
    return lax.ppermute(array, ("row", "col"), perm)


def place():
    row, col = lax.axis_index("row"), lax.axis_index("col")
    return lax.rem(row, ZH), col // (ZL * CORE), lax.rem(col // CORE, ZL), lax.rem(col, CORE)


def integrals_kernel(*refs):
    pieces, (own_ref, other_ref, own_out, other_out) = refs[:-4], refs[-4:]
    zh, _, zl, _ = place()
    swapped = [lax.rem((zh * ZL + zl + step) // ZL, ZH) != 0 for step in range(ZL)]
    rows = []
    for dy in range(Y):
        held = {}
        for g, group in enumerate(GROUPS):
            for i, dz in enumerate(group):
                held[dz] = pieces[dy * len(GROUPS) + g][i, 0]
        for step in range(ZL):
            near, far = held[step], held[step + ZL]
            low = jnp.where(swapped[step], far, near)
            high = jnp.where(swapped[step], near, far)
            rows.append(jnp.concatenate([low, high], axis=1))
    window = jnp.concatenate(rows, axis=0)
    for vectors_ref, out_ref in ((own_ref, own_out), (other_ref, other_out)):
        block = jnp.dot(vectors_ref[...], window, preferred_element_type=jnp.float32)
        out_ref[...] = block.astype(out_ref.dtype)


def integrals_of(pieces, own, other):
    _, n_a, q_part, c_part = pieces[0].shape
    rows, n_q = own.shape
    n_c = c_part * ZH
    specs = [
        pl.BlockSpec((piece.shape[0], 1, q_part, c_part), lambda a: (0, a, 0, 0)) for piece in pieces
    ]
    out = jax.ShapeDtypeStruct((rows, n_a * n_c), jnp.bfloat16)
    return pl.pallas_call(
        integrals_kernel,
        grid=(n_a,),
        out_shape=(out, out),
        in_specs=specs + [pl.BlockSpec((rows, n_q), lambda a: (0, 0))] * 2,
        out_specs=(pl.BlockSpec((rows, n_c), lambda a: (0, a)),) * 2,
        compiler_params=pltpu.CompilerParams(vmem_limit_bytes=24 << 20),
        cost_estimate=pl.CostEstimate(
            flops=4 * rows * n_q * n_a * n_c, transcendentals=0,
            bytes_accessed=2 * (n_q * n_a * n_c + 2 * rows * n_q + 2 * rows * n_a * n_c),
        ),
    )(*pieces, own, other)


def ladder_kernel(*refs, n_a, n_b, n_c, d_block):
    amps, sums, (out_ref, acc_ref) = refs[:-4], refs[-4:-2], refs[-2:]
    zh = place()[0]
    block = pl.program_id(0)

    @pl.when(block == 0)
    def _():
        acc_ref[...] = jnp.zeros_like(acc_ref)

    total = acc_ref[...]
    for half, integrals_ref in enumerate(sums):
        held = amps[half * ZH * X:(half + 1) * ZH * X]
        for d in range(d_block):
            near = jnp.concatenate([held[i][d] for i in range(X)], axis=0)
            far = jnp.concatenate([held[X + i][d] for i in range(X)], axis=0)
            low, high = jnp.where(zh != 0, far, near), jnp.where(zh != 0, near, far)
            amplitudes = jnp.concatenate([low, high], axis=0)
            stacked = jnp.concatenate(
                [integrals_ref[d * n_b:(d + 1) * n_b, a * n_c:(a + 1) * n_c] for a in range(n_a)], axis=0)
            total += jnp.dot(stacked, amplitudes, preferred_element_type=jnp.float32)
    acc_ref[...] = total

    @pl.when(block == pl.num_programs(0) - 1)
    def _():
        out_ref[...] = acc_ref[...].T.astype(out_ref.dtype)


def ladder_of(integrals, amps, n_a, d_block=4):
    near, far = amps
    n_d, c_part, n_n = far[0][0].shape
    steps = n_d // d_block
    n_c = c_part * X * ZH
    n_b = integrals[0].shape[0] // n_d

    def kernel(*refs):
        ladder_kernel(*refs, n_a=n_a, n_b=n_b, n_c=n_c, d_block=d_block)

    return pl.pallas_call(
        kernel,
        grid=(steps,),
        out_shape=jax.ShapeDtypeStruct((n_n, n_a * n_b), PARTIAL),
        in_specs=[pl.BlockSpec((d_block, c_part, n_n), lambda d: (d, 0, 0))] * (2 * X)
        + [pl.BlockSpec((d_block, c_part, n_n), lambda d: (d + steps, 0, 0))] * X
        + [pl.BlockSpec((d_block, c_part, n_n), lambda d: (d, 0, 0))] * X
        + [pl.BlockSpec((d_block * n_b, n_a * n_c), lambda d: (d, 0))] * 2,
        out_specs=pl.BlockSpec((n_n, n_a * n_b), lambda d: (0, 0)),
        scratch_shapes=[pltpu.VMEM((n_a * n_b, n_n), jnp.float32)],
        compiler_params=pltpu.CompilerParams(vmem_limit_bytes=24 << 20),
        cost_estimate=pl.CostEstimate(
            flops=4 * n_d * n_b * n_a * n_c * n_n, transcendentals=0,
            bytes_accessed=4 * (n_d * n_c * n_n + n_d * n_b * n_a * n_c),
        ),
    )(*near, *far[0], *near, *far[1], *integrals)


def ordered_vectors(pair_vectors):
    n_b, n_d, n_q = pair_vectors.shape
    _, y, zl, _ = place()
    part = n_q // (Y * ZL)
    position = jnp.arange(n_q)
    far, q = position // part, position % part
    source = ((y + far // ZL) % Y * ZL + (zl + far % ZL) % ZL) * part + q
    picked = (jnp.arange(n_q)[:, None] == source[None, :]).astype(pair_vectors.dtype)
    moved = pair_vectors.transpose(1, 0, 2).reshape(n_d * n_b, n_q)
    own = jnp.dot(moved, picked, preferred_element_type=jnp.float32).astype(pair_vectors.dtype)
    return own, fetch(own, dcore=1)


def kept_and_given(array, axis):
    low, high = jnp.split(array, 2, axis=axis)
    first = place()[3] == 0
    return jnp.where(first, low, high), jnp.where(first, high, low)


def gathered_window(window):
    mine = window.transpose(1, 2, 0)
    half = mine.shape[2] // 2
    near = [mine] + [fetch(mine, dx=dx) for dx in range(1, X)]
    parts = jnp.concatenate([m[..., :half] for m in near] + [m[..., half:] for m in near], axis=2)
    kept, given = kept_and_given(parts, 2)
    taken = fetch(given, dcore=1)
    first = place()[3] == 0
    parts = jnp.concatenate([jnp.where(first, kept, taken), jnp.where(first, taken, kept)], axis=1)
    along_z = {0: parts}
    for dz, source, step in ((1, 0, 1), (7, 0, 7), (2, 0, 2), (6, 0, 6), (3, 2, 1), (5, 6, 7), (4, 2, 2)):
        along_z[dz] = fetch(along_z[source], dz=step)
    pieces = []
    for g, group in enumerate(GROUPS):
        block = jnp.stack([along_z[dz] for dz in group])
        up, down = fetch(block, dy=1), fetch(block, dy=3)
        source, step = {1: (up, 1), 2: (down, 3)}.get(g, (block, 2))
        pieces.append([block, up, fetch(source, dy=step), down])
    return [pieces[g][dy] for dy in range(Y) for g in range(len(GROUPS))]


def gathered_amplitudes(amplitudes):
    kept, given = kept_and_given(amplitudes.transpose(1, 0, 2), 1)
    taken = fetch(given, dcore=1)
    mine = jnp.concatenate([kept, taken], axis=0)
    near = [mine] + [fetch(mine, dx=dx) for dx in range(1, X)]
    far = []
    for part in (kept, taken):
        swap = fetch(part, dz=ZL)
        far.append([swap] + [fetch(swap, dx=dx) for dx in range(1, X)])
    return near, far


def local(chol_window, pair_vectors, amplitudes):
    n_b = pair_vectors.shape[0]
    n_a = chol_window.shape[1]
    n_n = amplitudes.shape[2]
    pieces = gathered_window(chol_window)
    amps = gathered_amplitudes(amplitudes)
    integrals = integrals_of(pieces, *ordered_vectors(pair_vectors))
    partial = ladder_of(integrals, amps, n_a)
    tiles = lax.all_to_all(partial.reshape(COLS, n_n // COLS, n_a * n_b), "col", 0, 0, tiled=True)
    total = jnp.sum(tiles.astype(jnp.float32), axis=0)
    return total.reshape(n_n // COLS, n_a, n_b).transpose(1, 0, 2)


def solution(mesh):
    return jax.shard_map(
        local,
        mesh=mesh,
        in_specs=(P("row", None, "col"), P("row", "col", None), P("row", "col", None)),
        out_specs=P(None, "col", "row"),
        check_vma=False,
    )
```
